8 devices in a mesh: dp: 2 (over z, y), tp: 4 (over x, core).
Axes of the slice: x: 2, y: 2, z: 1, core: 2. Of those that a mesh axis runs over, the one named last changes fastest.
Arguments:
- act_in: bfloat16 [512, 5120], P('dp'), parts along dimension 0
- w_qkv: bfloat16 [2, 5120, 40, 3, 128], P(None, None, 'tp')
- w_out: bfloat16 [2, 40, 128, 5120], P(None, 'tp')
- w_up: bfloat16 [2, 5120, 20480], P(None, None, 'tp')
- w_down: bfloat16 [2, 20480, 5120], P(None, 'tp')
- gain_one: float32 [2, 5120], replicated
- gain_two: float32 [2, 5120], replicated
Outputs:
- output: bfloat16 [512, 5120], P('dp'), parts along dimension 0
There are 2 independent parts. The reference program is written for one: setup_inputs(seed, part) draws one part's arguments, and reference() takes and returns one part's arrays. A program takes and returns all parts, laid end to end along the dimension named above; an argument that names none is the same for every part.
All inputs are finite; a program needn't handle non-finite values.
Results may differ from the reference program's by a relative error of at most 0.0152739.
Values are sent between devices in bfloat16 or wider.
A program may use at most 1.25 GiB of HBM per device.

```python
import math
import jax
import jax.numpy as jnp
from jax import lax

SEQ_LEN = 256
MODEL_DIM = 5120
NUM_HEADS = 40
FFN_DIM = 20480
NUM_LAYERS = 2

HEAD_DIM = MODEL_DIM // NUM_HEADS
SCORE_SCALE = 1.0 / math.sqrt(HEAD_DIM)
ROW_BLOCK = math.gcd(SEQ_LEN, 2 ** int(math.log2(max(8, 2 ** 24 // (NUM_HEADS * SEQ_LEN)))))


def setup_inputs(seed: int = 0, part: int = 0) -> dict:
    part_key = jax.random.fold_in(jax.random.key(seed), part)
    key_common, key_noise = jax.random.split(part_key)
    shared_mean = jax.random.normal(key_common, (1, MODEL_DIM), jnp.float32)
    token_noise = jax.random.normal(key_noise, (SEQ_LEN, MODEL_DIM), jnp.float32)
    weight_keys = jax.random.split(jax.random.key(seed + 1), 6)
    w_qkv = jax.random.normal(weight_keys[0], (NUM_LAYERS, MODEL_DIM, NUM_HEADS, 3, HEAD_DIM), jnp.float32) * MODEL_DIM ** -0.5
    w_out = jax.random.normal(weight_keys[1], (NUM_LAYERS, NUM_HEADS, HEAD_DIM, MODEL_DIM), jnp.float32) * MODEL_DIM ** -0.5
    w_up = jax.random.normal(weight_keys[2], (NUM_LAYERS, MODEL_DIM, FFN_DIM), jnp.float32) * MODEL_DIM ** -0.5
    w_down = jax.random.normal(weight_keys[3], (NUM_LAYERS, FFN_DIM, MODEL_DIM), jnp.float32) * FFN_DIM ** -0.5
    gain_one = jax.random.uniform(weight_keys[4], (NUM_LAYERS, MODEL_DIM), jnp.float32, 0.5, 1.5)
    gain_two = jax.random.uniform(weight_keys[5], (NUM_LAYERS, MODEL_DIM), jnp.float32, 0.5, 1.5)
    return {
        "act_in": (shared_mean + token_noise).astype(jnp.bfloat16),
        "w_qkv": w_qkv.astype(jnp.bfloat16),
        "w_out": w_out.astype(jnp.bfloat16),
        "w_up": w_up.astype(jnp.bfloat16),
        "w_down": w_down.astype(jnp.bfloat16),
        "gain_one": gain_one,
        "gain_two": gain_two,
    }


def layer_norm(act_rows, gain_vec):
    rows_f32 = act_rows.astype(jnp.float32)
    centred = rows_f32 - jnp.mean(rows_f32, axis=-1, keepdims=True)
    var_rows = jnp.mean(centred * centred, axis=-1, keepdims=True)
    return (centred * lax.rsqrt(var_rows + 1e-5) * gain_vec).astype(jnp.bfloat16)


def causal_attention(query_rows, key_rows, value_rows):
    key_pos = jnp.arange(SEQ_LEN)
    key_f32 = key_rows.astype(jnp.float32)
    value_f32 = value_rows.astype(jnp.float32)

    def one_block(blk_idx):
        row_start = blk_idx * ROW_BLOCK
        q_blk = lax.dynamic_slice_in_dim(query_rows, row_start, ROW_BLOCK, axis=0).astype(jnp.float32)
        scores = jnp.einsum("qhd,khd->hqk", q_blk, key_f32) * SCORE_SCALE
        q_pos = row_start + jnp.arange(ROW_BLOCK)
        scores = jnp.where(key_pos[None, None, :] <= q_pos[None, :, None], scores, -1e30)
        exp_scores = jnp.exp(scores - jnp.max(scores, axis=-1, keepdims=True))
        prob_sum = jnp.sum(exp_scores, axis=-1)
        mix_out = jnp.einsum("hqk,khd->qhd", exp_scores.astype(jnp.bfloat16).astype(jnp.float32), value_f32)
        return (mix_out / prob_sum.T[:, :, None]).astype(jnp.bfloat16)

    blocks = lax.map(one_block, jnp.arange(SEQ_LEN // ROW_BLOCK))
    return blocks.reshape(SEQ_LEN, NUM_HEADS, HEAD_DIM)


def reference(act_in, w_qkv, w_out, w_up, w_down, gain_one, gain_two):
    def layer_step(act_rows, layer_weights):
        qkv_mat, out_mat, up_mat, down_mat, norm_one, norm_two = layer_weights
        normed = layer_norm(act_rows, norm_one)
        qkv_rows = jnp.dot(normed, qkv_mat.reshape(MODEL_DIM, 3 * MODEL_DIM), preferred_element_type=jnp.float32).astype(jnp.bfloat16)
        qkv_rows = qkv_rows.reshape(SEQ_LEN, NUM_HEADS, 3, HEAD_DIM)
        attn_rows = causal_attention(qkv_rows[:, :, 0], qkv_rows[:, :, 1], qkv_rows[:, :, 2])
        branch = jnp.dot(attn_rows.reshape(SEQ_LEN, MODEL_DIM), out_mat.reshape(MODEL_DIM, MODEL_DIM), preferred_element_type=jnp.float32)
        act_rows = (act_rows.astype(jnp.float32) + branch).astype(jnp.bfloat16)
        normed = layer_norm(act_rows, norm_two)
        hidden = jax.nn.gelu(jnp.dot(normed, up_mat, preferred_element_type=jnp.float32), approximate=True).astype(jnp.bfloat16)
        branch = jnp.dot(hidden, down_mat, preferred_element_type=jnp.float32)
        act_rows = (act_rows.astype(jnp.float32) + branch).astype(jnp.bfloat16)
        return act_rows, None

    final_rows = lax.scan(layer_step, act_in, (w_qkv, w_out, w_up, w_down, gain_one, gain_two))[0]
    return final_rows
```

```python
import functools
import math
import jax
import jax.numpy as jnp
from jax import lax
from jax.experimental import pallas as pl
from jax.experimental.pallas import tpu as pltpu
from jax.sharding import PartitionSpec as P

MESH = pl.DeviceIdType.MESH
F32, BF16 = jnp.float32, jnp.bfloat16
WID = 512
LAG_X = 4
LAG_USE = 5
A_SLOTS, B_SLOTS, C_SLOTS = 3, 3, 4


def layer_kernel(
    num_layers, seq, dim, heads, hd, ffn,
    x_hbm, wqkv, wo, w1, w2, g1_ref, g2_ref, out_hbm,
    xs, acc, hid, part, recv_a, send_c, recv_c, ys, mean0, sum1, sum2,
    a_buf, b_buf, c_buf,
    x_sem, a_sem, b_sem, c_sem, o_sem, sa, ra, sc, rc, sd, rd,
):
    dp = lax.axis_index("dp")
    tp = lax.axis_index("tp")
    core = lax.rem(tp, 2)
    sib = (dp, tp + 1 - 2 * core)
    pair = (dp, lax.rem(tp + 2, 4))
    half = seq // 2
    mine = pl.ds(pl.multiple_of(core * half, half), half)
    other = pl.ds(pl.multiple_of((1 - core) * half, half), half)
    nc = dim // WID
    qkv_tiles, up_tiles = heads * 3 * hd // 256, ffn // 256
    o_off = heads * 3 * hd

    barrier = pltpu.get_barrier_semaphore()
    for peer in (sib, pair):
        pl.semaphore_signal(barrier, inc=1, device_id=peer, device_id_type=MESH)
    pl.semaphore_wait(barrier, 2)

    def rows(j):
        return pl.ds(pl.multiple_of(j * WID, WID), WID)

    def x_copy(j):
        return pltpu.make_async_copy(x_hbm.at[:, rows(j)], xs.at[j], x_sem.at[j])

    def out_copy(j):
        return pltpu.make_async_copy(xs.at[j], out_hbm.at[:, rows(j)], o_sem.at[j])

    def a_start(stage, j):
        layer, is_up = stage // 2, stage % 2
        if stage >= 2 * num_layers:
            return
        slot = lax.rem(stage * nc + j, A_SLOTS)
        if is_up:
            def one(t, carry):
                cols = pl.ds(pl.multiple_of(t * 256, 256), 256)
                pltpu.make_async_copy(
                    w1.at[layer, rows(j), cols], a_buf.at[slot, t], a_sem.at[slot]
                ).start()
                return carry
            lax.fori_loop(0, up_tiles, one, 0)
        else:
            for s in range(2):
                pltpu.make_async_copy(
                    wqkv.at[layer, :, s, rows(j), :],
                    a_buf.at[slot, pl.ds(0, qkv_tiles), :, pl.ds(s * 128, 128)],
                    a_sem.at[slot],
                ).start()

    def a_next(stage, j):
        @pl.when(j + A_SLOTS < nc)
        def _():
            a_start(stage, j + A_SLOTS)

        @pl.when(j + A_SLOTS >= nc)
        def _():
            a_start(stage + 1, j + A_SLOTS - nc)

    def a_wait(stage, j):
        slot = lax.rem(stage * nc + j, A_SLOTS)
        tiles = up_tiles if stage % 2 else qkv_tiles
        view = a_buf.at[slot, pl.ds(0, tiles)]
        pltpu.make_async_copy(view, view, a_sem.at[slot]).wait()
        return slot

    def b_copy(layer, j):
        slot = lax.rem(layer * nc + j, B_SLOTS)
        return slot, pltpu.make_async_copy(
            w2.at[layer, :, rows(j)], b_buf.at[slot], b_sem.at[slot])

    def c_copy(layer, j):
        slot = lax.rem(layer * nc + j, C_SLOTS)
        return slot, pltpu.make_async_copy(
            wo.at[layer, :, rows(j)], c_buf.at[slot], c_sem.at[slot])

    def ring_next(copy, slots, layer, j):
        @pl.when(j + slots < nc)
        def _():
            copy(layer, j + slots)[1].start()

        if layer + 1 < num_layers:
            @pl.when(j + slots >= nc)
            def _():
                copy(layer + 1, j + slots - nc)[1].start()

    def use(stage, j):
        layer, is_up = stage // 2, stage % 2
        gain_ref = g2_ref if is_up else g1_ref
        gain = gain_ref[pl.ds(layer, 1), rows(j)]
        xc = xs[j].astype(F32)

        @pl.when(j == 0)
        def _():
            m = jnp.mean(xc, axis=1, keepdims=True)
            mean0[...] = jnp.broadcast_to(m, mean0.shape)
            sum1[...] = jnp.zeros_like(sum1)
            sum2[...] = jnp.zeros_like(sum2)
            acc[...] = jnp.zeros_like(acc)

        shift = mean0[...]
        s1, s2 = sum1[...], sum2[...]
        for t in range(WID // 128):
            cols = slice(t * 128, (t + 1) * 128)
            d = xs[j, :, cols].astype(F32) - shift
            s1 = s1 + d
            s2 = s2 + d * d
            ys[0:seq, cols] = (d * gain[:, cols]).astype(BF16)
        sum1[...] = s1
        sum2[...] = s2
        g_hi = gain.astype(BF16)
        g_lo = (gain - g_hi.astype(F32)).astype(BF16)
        row = lax.broadcasted_iota(jnp.int32, (16, WID), 0)
        hi = jnp.broadcast_to(g_hi.astype(F32), (16, WID))
        lo = jnp.broadcast_to(g_lo.astype(F32), (16, WID))
        extra = jnp.where(row == 0, hi, jnp.where(row == 1, lo, 0.0))
        ys[seq:seq + 16, :] = extra.astype(BF16)

        slot = a_wait(stage, j)
        lhs = ys[...]
        for t in range(up_tiles if is_up else qkv_tiles):
            cols = slice(t * 256, (t + 1) * 256)
            acc[:, cols] += jnp.dot(lhs, a_buf[slot, t], preferred_element_type=F32)
        a_next(stage, j)

    def use_end(stage):
        is_up = stage % 2
        delta = jnp.sum(sum1[...], axis=1, keepdims=True) * (1.0 / dim)
        var = jnp.sum(sum2[...], axis=1, keepdims=True) * (1.0 / dim) - delta * delta
        rstd = lax.rsqrt(jnp.maximum(var, 0.0) + 1e-5)

        def one(t, carry):
            cols = pl.ds(pl.multiple_of(t * 256, 256), 256)
            colsum = acc[seq:seq + 1, cols] + acc[seq + 1:seq + 2, cols]
            val = (acc[0:seq, cols] - delta * colsum) * rstd
            if is_up:
                val = jax.nn.gelu(val, approximate=True)
            hid[:, cols] = val.astype(BF16)
            return carry

        lax.fori_loop(0, up_tiles if is_up else qkv_tiles, one, 0)

    def attention():
        q_pos = lax.broadcasted_iota(jnp.int32, (seq, seq), 0)
        k_pos = lax.broadcasted_iota(jnp.int32, (seq, seq), 1)
        keep = k_pos <= q_pos
        scale = 1.0 / math.sqrt(hd)
        for h in range(heads):
            base = 3 * h * hd
            q = hid[:, base:base + hd]
            k = hid[:, base + hd:base + 2 * hd]
            v = hid[:, base + 2 * hd:base + 3 * hd]
            s = lax.dot_general(q, k, (((1,), (1,)), ((), ())), preferred_element_type=F32) * scale
            s = jnp.where(keep, s, -1e30)
            e = jnp.exp(s - jnp.max(s, axis=1, keepdims=True))
            total = jnp.sum(e, axis=1, keepdims=True)
            mix = jnp.dot(e.astype(BF16), v, preferred_element_type=F32)
            hid[:, o_off + h * hd:o_off + (h + 1) * hd] = (mix / total).astype(BF16)

    def make_out(layer, j):
        slot, copy = c_copy(layer, j)
        copy.wait()
        part[j] = jnp.dot(hid[:, o_off:], c_buf[slot], preferred_element_type=F32).astype(BF16)
        ring_next(c_copy, C_SLOTS, layer, j)

    def make_down(layer, j):
        slot, copy = b_copy(layer, j)
        copy.wait()
        part[j] = jnp.dot(hid[...], b_buf[slot], preferred_element_type=F32).astype(BF16)
        ring_next(b_copy, B_SLOTS, layer, j)

    def window(index, make, consume):
        par = index % 2

        def a_send(j):
            return pltpu.make_async_remote_copy(
                part.at[j, other], recv_a.at[par, j], sa.at[j], ra.at[par, j],
                device_id=sib, device_id_type=MESH)

        def c_send(j):
            return pltpu.make_async_remote_copy(
                send_c.at[j], recv_c.at[par, j], sc.at[j], rc.at[par, j],
                device_id=pair, device_id_type=MESH)

        def d_send(j):
            return pltpu.make_async_remote_copy(
                xs.at[j, mine], xs.at[j, mine], sd.at[j], rd.at[par, j],
                device_id=sib, device_id_type=MESH)

        def d_recv(j):
            return pltpu.make_async_remote_copy(
                xs.at[j, other], xs.at[j, other], sd.at[j], rd.at[par, j],
                device_id=sib, device_id_type=MESH)

        def step(i, carry):
            @pl.when(i < nc)
            def _():
                make(i)
                a_send(i).start()

            @pl.when(jnp.logical_and(i >= 1, i < nc + 1))
            def _():
                j = i - 1
                a_send(j).wait_recv()
                send_c[j] = (part[j, mine, :].astype(F32) + recv_a[par, j].astype(F32)).astype(BF16)
                c_send(j).start()

            @pl.when(jnp.logical_and(i >= LAG_X, i < nc + LAG_X))
            def _():
                j = i - LAG_X
                c_send(j).wait_recv()
                total = send_c[j].astype(F32) + recv_c[par, j].astype(F32)
                xs[j, mine, :] = (xs[j, mine, :].astype(F32) + total).astype(BF16)
                d_send(j).start()

            @pl.when(i >= LAG_USE)
            def _():
                j = i - LAG_USE
                a_send(j).wait_send()
                c_send(j).wait_send()
                d_send(j).wait_send()
                d_recv(j).wait_recv()
                consume(j)
            return carry

        lax.fori_loop(0, nc + LAG_USE, step, 0)

    for j in range(nc):
        x_copy(j).start()
    for j in range(A_SLOTS):
        a_start(0, j)

    def first(j, carry):
        x_copy(j).wait()
        use(0, j)
        return carry

    lax.fori_loop(0, nc, first, 0)
    for j in range(C_SLOTS):
        c_copy(0, j)[1].start()
    use_end(0)
    attention()
    for j in range(B_SLOTS):
        b_copy(0, j)[1].start()

    for layer in range(num_layers):
        window(2 * layer, functools.partial(make_out, layer), functools.partial(use, 2 * layer + 1))
        use_end(2 * layer + 1)
        if layer + 1 < num_layers:
            window(2 * layer + 1, functools.partial(make_down, layer), functools.partial(use, 2 * layer + 2))
            use_end(2 * layer + 2)
            attention()
        else:
            window(2 * layer + 1, functools.partial(make_down, layer), lambda j: out_copy(j).start())

    def last(j, carry):
        out_copy(j).wait()
        return carry

    lax.fori_loop(0, nc, last, 0)


def solution(mesh):
    def device_fn(act_in, w_qkv, w_out, w_up, w_down, gain_one, gain_two):
        seq, dim = act_in.shape
        num_layers, _, heads, _, hd = w_qkv.shape
        ffn = w_up.shape[2]
        nc = dim // WID
        wq = jnp.transpose(w_qkv, (0, 2, 3, 1, 4)).reshape(num_layers, heads * 3 // 2, 2, dim, hd)
        wo = w_out.reshape(num_layers, heads * hd, dim)
        any_spec = pl.BlockSpec(memory_space=pl.ANY)
        vmem_spec = pl.BlockSpec(memory_space=pltpu.VMEM)
        return pl.pallas_call(
            functools.partial(layer_kernel, num_layers, seq, dim, heads, hd, ffn),
            out_shape=jax.ShapeDtypeStruct((seq, dim), BF16),
            in_specs=[any_spec] * 5 + [vmem_spec] * 2,
            out_specs=any_spec,
            scratch_shapes=[
                pltpu.VMEM((nc, seq, WID), BF16),
                pltpu.VMEM((seq + 16, ffn), F32),
                pltpu.VMEM((seq, ffn), BF16),
                pltpu.VMEM((nc, seq, WID), BF16),
                pltpu.VMEM((2, nc, seq // 2, WID), BF16),
                pltpu.VMEM((nc, seq // 2, WID), BF16),
                pltpu.VMEM((2, nc, seq // 2, WID), BF16),
                pltpu.VMEM((seq + 16, WID), BF16),
                pltpu.VMEM((seq, 128), F32),
                pltpu.VMEM((seq, 128), F32),
                pltpu.VMEM((seq, 128), F32),
                pltpu.VMEM((A_SLOTS, ffn // 256, WID, 256), BF16),
                pltpu.VMEM((B_SLOTS, ffn, WID), BF16),
                pltpu.VMEM((C_SLOTS, heads * hd, WID), BF16),
                pltpu.SemaphoreType.DMA((nc,)),
                pltpu.SemaphoreType.DMA((A_SLOTS,)),
                pltpu.SemaphoreType.DMA((B_SLOTS,)),
                pltpu.SemaphoreType.DMA((C_SLOTS,)),
                pltpu.SemaphoreType.DMA((nc,)),
                pltpu.SemaphoreType.DMA((nc,)),
                pltpu.SemaphoreType.DMA((2, nc)),
                pltpu.SemaphoreType.DMA((nc,)),
                pltpu.SemaphoreType.DMA((2, nc)),
                pltpu.SemaphoreType.DMA((nc,)),
                pltpu.SemaphoreType.DMA((2, nc)),
            ],
            compiler_params=pltpu.CompilerParams(
                collective_id=0, has_side_effects=True, vmem_limit_bytes=67_000_000),
            name="layers",
        )(act_in, wq, wo, w_up, w_down, gain_one, gain_two)

    return jax.shard_map(
        device_fn,
        mesh=mesh,
        in_specs=(
            P("dp", None),
            P(None, None, "tp", None, None),
            P(None, "tp", None, None),
            P(None, None, "tp"),
            P(None, "tp", None),
            P(None, None),
            P(None, None),
        ),
        out_specs=P("dp", None),
        check_vma=False,
    )
```

```python
import functools
import math
import jax
import jax.numpy as jnp
from jax import lax
from jax.experimental import pallas as pl
from jax.experimental.pallas import tpu as pltpu
from jax.sharding import PartitionSpec as P

MESH = pl.DeviceIdType.MESH
F32, BF16 = jnp.float32, jnp.bfloat16
WID = 512
GAIN = 16
LAG_X = 4
LAG_USE = 5
GELU_A = math.sqrt(2.0 / math.pi)
GELU_B = 0.044715 * GELU_A
A_SLOTS, B_SLOTS, C_SLOTS = 3, 3, 4


def layer_kernel(
    num_layers, seq, dim, heads, hd, ffn,
    x_hbm, wqkv, wo, w1, w2, g1_hbm, g2_hbm, out_hbm,
    g1_ref, g2_ref, xs, acc, hid, part, recv_a, send_c, recv_c, ys0, ys1, mean0, sum1, sum2,
    a_buf, b_buf, c_buf,
    g_sem, x_sem, a_sem, b_sem, c_sem, o_sem, sa, ra, sc, rc, sd, rd,
):
    dp = lax.axis_index("dp")
    tp = lax.axis_index("tp")
    core = lax.rem(tp, 2)
    sib = (dp, tp + 1 - 2 * core)
    pair = (dp, lax.rem(tp + 2, 4))
    half = seq // 2
    mine = pl.ds(pl.multiple_of(core * half, half), half)
    other = pl.ds(pl.multiple_of((1 - core) * half, half), half)
    nc = dim // WID
    qkv_tiles, up_tiles = heads * 3 * hd // 256, ffn // 256
    o_off = heads * 3 * hd

    barrier = pltpu.get_barrier_semaphore()
    for peer in (sib, pair):
        pl.semaphore_signal(barrier, inc=1, device_id=peer, device_id_type=MESH)

    def rows(j):
        return pl.ds(pl.multiple_of(j * WID, WID), WID)

    def x_copy(j):
        return pltpu.make_async_copy(x_hbm.at[:, rows(j)], xs.at[j], x_sem.at[j])

    def out_copy(j):
        return pltpu.make_async_copy(xs.at[j], out_hbm.at[:, rows(j)], o_sem.at[j])

    def a_start(stage, j):
        layer, is_up = stage // 2, stage % 2
        if stage >= 2 * num_layers:
            return
        slot = lax.rem(stage * nc + j, A_SLOTS)
        if is_up:
            def one(t, carry):
                cols = pl.ds(pl.multiple_of(t * 256, 256), 256)
                pltpu.make_async_copy(
                    w1.at[layer, rows(j), cols], a_buf.at[slot, t], a_sem.at[slot]
                ).start(priority=1)
                return carry
            lax.fori_loop(0, up_tiles, one, 0)
        else:
            for s in range(2):
                pltpu.make_async_copy(
                    wqkv.at[layer, :, s, rows(j), :],
                    a_buf.at[slot, pl.ds(0, qkv_tiles), :, pl.ds(s * 128, 128)],
                    a_sem.at[slot],
                ).start(priority=1)

    def a_next(stage, j):
        @pl.when(j + A_SLOTS < nc)
        def _():
            a_start(stage, j + A_SLOTS)

        @pl.when(j + A_SLOTS >= nc)
        def _():
            a_start(stage + 1, j + A_SLOTS - nc)

    def a_wait(stage, j):
        slot = lax.rem(stage * nc + j, A_SLOTS)
        tiles = up_tiles if stage % 2 else qkv_tiles
        view = a_buf.at[slot, pl.ds(0, tiles)]
        pltpu.make_async_copy(view, view, a_sem.at[slot]).wait()
        return slot

    def b_copy(layer, j):
        slot = lax.rem(layer * nc + j, B_SLOTS)
        return slot, pltpu.make_async_copy(
            w2.at[layer, :, rows(j)], b_buf.at[slot], b_sem.at[slot])

    def c_copy(layer, j):
        slot = lax.rem(layer * nc + j, C_SLOTS)
        return slot, pltpu.make_async_copy(
            wo.at[layer, :, rows(j)], c_buf.at[slot], c_sem.at[slot])

    def ring_next(copy, slots, priority, layer, j):
        @pl.when(j + slots < nc)
        def _():
            copy(layer, j + slots)[1].start(priority=priority)

        if layer + 1 < num_layers:
            @pl.when(j + slots >= nc)
            def _():
                copy(layer + 1, j + slots - nc)[1].start(priority=priority)

    def prep_start(j):
        m = jnp.mean(xs[j].astype(F32), axis=1, keepdims=True)
        mean0[...] = jnp.broadcast_to(m, mean0.shape)
        sum1[...] = jnp.zeros_like(sum1)
        sum2[...] = jnp.zeros_like(sum2)

    def prep(stage, j, y_ref):
        layer, is_up = stage // 2, stage % 2
        gain_ref = g2_ref if is_up else g1_ref
        gain = gain_ref[pl.ds(layer, 1), rows(j)]
        shift = mean0[...]
        s1, s2 = sum1[...], sum2[...]
        for t in range(WID // 128):
            cols = slice(t * 128, (t + 1) * 128)
            d = xs[j, :, cols].astype(F32) - shift
            s1 = s1 + d
            s2 = s2 + d * d
            y_ref[GAIN:, cols] = (d * gain[:, cols]).astype(BF16)
        sum1[...] = s1
        sum2[...] = s2
        g_hi = gain.astype(BF16)
        g_lo = (gain - g_hi.astype(F32)).astype(BF16)
        row = lax.broadcasted_iota(jnp.int32, (GAIN, WID), 0)
        hi = jnp.broadcast_to(g_hi.astype(F32), (GAIN, WID))
        lo = jnp.broadcast_to(g_lo.astype(F32), (GAIN, WID))
        extra = jnp.where(row == 0, hi, jnp.where(row == 1, lo, 0.0))
        y_ref[0:GAIN, :] = extra.astype(BF16)

    def mul(stage, slot, y_ref):
        lhs = y_ref[...]
        for t in range(up_tiles if stage % 2 else qkv_tiles):
            cols = slice(t * 256, (t + 1) * 256)
            acc[:, cols] += jnp.dot(lhs, a_buf[slot, t], preferred_element_type=F32)

    def mul_last(stage, slot, y_ref):
        is_up = stage % 2
        delta = jnp.sum(sum1[...], axis=1, keepdims=True) * (1.0 / dim)
        var = jnp.sum(sum2[...], axis=1, keepdims=True) * (1.0 / dim) - delta * delta
        rstd = lax.rsqrt(jnp.maximum(var, 0.0) + 1e-5)
        back = delta * rstd
        lhs = y_ref[...]
        for t in range(up_tiles if is_up else qkv_tiles):
            cols = slice(t * 256, (t + 1) * 256)
            full = acc[:, cols] + jnp.dot(lhs, a_buf[slot, t], preferred_element_type=F32)
            colsum = full[0:1] + full[1:2]
            val = full[GAIN:] * rstd - back * colsum
            if is_up:
                inner = val * (GELU_A + GELU_B * (val * val))
                hv = 0.5 * val
                val = hv + hv * jnp.tanh(inner)
            hid[:, cols] = val.astype(BF16)

    def use(stage, j):
        @pl.when(j == 0)
        def _():
            prep_start(j)

        prep(stage, j, ys0)
        slot = a_wait(stage, j)

        @pl.when(j < nc - 1)
        def _():
            mul(stage, slot, ys0)

        @pl.when(j == nc - 1)
        def _():
            mul_last(stage, slot, ys0)

        a_next(stage, j)

    def attention():
        q_pos = lax.broadcasted_iota(jnp.int32, (seq, seq), 0)
        k_pos = lax.broadcasted_iota(jnp.int32, (seq, seq), 1)
        keep = k_pos <= q_pos
        scale = 1.0 / math.sqrt(hd)
        for h in range(heads):
            base = 3 * h * hd
            q = hid[:, base:base + hd]
            k = hid[:, base + hd:base + 2 * hd]
            v = hid[:, base + 2 * hd:base + 3 * hd]
            s = lax.dot_general(q, k, (((1,), (1,)), ((), ())), preferred_element_type=F32) * scale
            s = jnp.where(keep, s, -1e30)
            e = jnp.exp(s - jnp.max(s, axis=1, keepdims=True))
            total = jnp.sum(e, axis=1, keepdims=True)
            mix = jnp.dot(e.astype(BF16), v, preferred_element_type=F32)
            hid[:, o_off + h * hd:o_off + (h + 1) * hd] = (mix / total).astype(BF16)

    def make_out(layer, j):
        slot, copy = c_copy(layer, j)
        copy.wait()
        part[j] = jnp.dot(hid[:, o_off:], c_buf[slot], preferred_element_type=F32).astype(BF16)
        ring_next(c_copy, C_SLOTS, 0, layer, j)

    def make_down(layer, j):
        slot, copy = b_copy(layer, j)
        copy.wait()
        part[j] = jnp.dot(hid[...], b_buf[slot], preferred_element_type=F32).astype(BF16)
        ring_next(b_copy, B_SLOTS, 1, layer, j)

    def window(index, make, consume, zero_acc=True):
        par = index % 2

        def a_send(j):
            return pltpu.make_async_remote_copy(
                part.at[j, other], recv_a.at[par, j], sa.at[j], ra.at[par, j],
                device_id=sib, device_id_type=MESH)

        def c_send(j):
            return pltpu.make_async_remote_copy(
                send_c.at[j], recv_c.at[par, j], sc.at[j], rc.at[par, j],
                device_id=pair, device_id_type=MESH)

        def d_send(j):
            return pltpu.make_async_remote_copy(
                xs.at[j, mine], xs.at[j, mine], sd.at[j], rd.at[par, j],
                device_id=sib, device_id_type=MESH)

        def d_recv(j):
            return pltpu.make_async_remote_copy(
                xs.at[j, other], xs.at[j, other], sd.at[j], rd.at[par, j],
                device_id=sib, device_id_type=MESH)

        def pair_sum(j):
            a_send(j).wait_recv()
            send_c[j] = (part[j, mine, :].astype(F32) + recv_a[par, j].astype(F32)).astype(BF16)
            c_send(j).start()

        def step(i, carry):
            @pl.when(i < nc)
            def _():
                make(i)
                a_send(i).start()

            @pl.when(i == 0)
            def _():
                if zero_acc:
                    acc[...] = jnp.zeros_like(acc)
                pair_sum(0)

            @pl.when(jnp.logical_and(i >= 2, i < nc + 1))
            def _():
                pair_sum(i - 1)

            @pl.when(jnp.logical_and(i >= LAG_X, i < nc + LAG_X))
            def _():
                j = i - LAG_X
                c_send(j).wait_recv()
                total = send_c[j].astype(F32) + recv_c[par, j].astype(F32)
                xs[j, mine, :] = (xs[j, mine, :].astype(F32) + total).astype(BF16)
                d_send(j).start()

            @pl.when(i >= LAG_USE)
            def _():
                j = i - LAG_USE
                a_send(j).wait_send()
                c_send(j).wait_send()
                d_send(j).wait_send()
                d_recv(j).wait_recv()
                consume(j)
            return carry

        lax.fori_loop(0, nc + LAG_USE, step, 0)

    x_copy(0).start()
    g_copies = [pltpu.make_async_copy(src, dst, g_sem.at[n])
                for n, (src, dst) in enumerate(((g1_hbm, g1_ref), (g2_hbm, g2_ref)))]
    for copy in g_copies:
        copy.start()
    a_start(0, 0)
    for j in range(1, nc):
        x_copy(j).start()
    for j in range(1, A_SLOTS):
        a_start(0, j)
    acc[...] = jnp.zeros_like(acc)
    for copy in g_copies:
        copy.wait()
    x_copy(0).wait()
    prep_start(0)
    prep(0, 0, ys0)

    def first(j, now, then):
        x_copy(j + 1).wait()
        slot = a_wait(0, j)
        prep(0, j + 1, then)
        mul(0, slot, now)
        a_next(0, j)

    def first_two(i, carry):
        first(2 * i, ys0, ys1)
        first(2 * i + 1, ys1, ys0)
        return carry

    lax.fori_loop(0, nc // 2 - 1, first_two, 0)
    for n in range(C_SLOTS):
        c_copy(0, n)[1].start()
    first(nc - 2, ys0, ys1)
    mul_last(0, a_wait(0, nc - 1), ys1)
    a_next(0, nc - 1)
    attention()
    for j in range(B_SLOTS):
        b_copy(0, j)[1].start(priority=1)
    pl.semaphore_wait(barrier, 2)

    for layer in range(num_layers):
        window(2 * layer, functools.partial(make_out, layer), functools.partial(use, 2 * layer + 1))
        if layer + 1 < num_layers:
            window(2 * layer + 1, functools.partial(make_down, layer), functools.partial(use, 2 * layer + 2))
            attention()
        else:
            window(2 * layer + 1, functools.partial(make_down, layer), lambda j: out_copy(j).start(), False)

    def last(j, carry):
        out_copy(j).wait()
        return carry

    lax.fori_loop(0, nc, last, 0)


def solution(mesh):
    def device_fn(act_in, w_qkv, w_out, w_up, w_down, gain_one, gain_two):
        seq, dim = act_in.shape
        num_layers, _, heads, _, hd = w_qkv.shape
        ffn = w_up.shape[2]
        nc = dim // WID
        wq = jnp.transpose(w_qkv, (0, 2, 3, 1, 4)).reshape(num_layers, heads * 3 // 2, 2, dim, hd)
        wo = w_out.reshape(num_layers, heads * hd, dim)
        any_spec = pl.BlockSpec(memory_space=pl.ANY)
        return pl.pallas_call(
            functools.partial(layer_kernel, num_layers, seq, dim, heads, hd, ffn),
            out_shape=jax.ShapeDtypeStruct((seq, dim), BF16),
            in_specs=[any_spec] * 7,
            out_specs=any_spec,
            scratch_shapes=[
                pltpu.VMEM((num_layers, dim), F32),
                pltpu.VMEM((num_layers, dim), F32),
                pltpu.VMEM((nc, seq, WID), BF16),
                pltpu.VMEM((seq + GAIN, ffn), F32),
                pltpu.VMEM((seq, ffn), BF16),
                pltpu.VMEM((nc, seq, WID), BF16),
                pltpu.VMEM((2, nc, seq // 2, WID), BF16),
                pltpu.VMEM((nc, seq // 2, WID), BF16),
                pltpu.VMEM((2, nc, seq // 2, WID), BF16),
                pltpu.VMEM((seq + GAIN, WID), BF16),
                pltpu.VMEM((seq + GAIN, WID), BF16),
                pltpu.VMEM((seq, 128), F32),
                pltpu.VMEM((seq, 128), F32),
                pltpu.VMEM((seq, 128), F32),
                pltpu.VMEM((A_SLOTS, ffn // 256, WID, 256), BF16),
                pltpu.VMEM((B_SLOTS, ffn, WID), BF16),
                pltpu.VMEM((C_SLOTS, heads * hd, WID), BF16),
                pltpu.SemaphoreType.DMA((2,)),
                pltpu.SemaphoreType.DMA((nc,)),
                pltpu.SemaphoreType.DMA((A_SLOTS,)),
                pltpu.SemaphoreType.DMA((B_SLOTS,)),
                pltpu.SemaphoreType.DMA((C_SLOTS,)),
                pltpu.SemaphoreType.DMA((nc,)),
                pltpu.SemaphoreType.DMA((nc,)),
                pltpu.SemaphoreType.DMA((2, nc)),
                pltpu.SemaphoreType.DMA((nc,)),
                pltpu.SemaphoreType.DMA((2, nc)),
                pltpu.SemaphoreType.DMA((nc,)),
                pltpu.SemaphoreType.DMA((2, nc)),
            ],
            compiler_params=pltpu.CompilerParams(
                collective_id=0, has_side_effects=True, vmem_limit_bytes=67_000_000),
            name="layers",
        )(act_in, wq, wo, w_up, w_down, gain_one, gain_two)

    return jax.shard_map(
        device_fn,
        mesh=mesh,
        in_specs=(
            P("dp", None),
            P(None, None, "tp", None, None),
            P(None, "tp", None, None),
            P(None, None, "tp"),
            P(None, "tp", None),
            P(None, None),
            P(None, None),
        ),
        out_specs=P("dp", None),
        check_vma=False,
    )
```

```python
import functools
import math
import jax
import jax.numpy as jnp
from jax import lax
from jax.experimental import pallas as pl
from jax.experimental.pallas import tpu as pltpu
from jax.sharding import PartitionSpec as P

MESH = pl.DeviceIdType.MESH
F32, BF16 = jnp.float32, jnp.bfloat16
WID = 512
GAIN = 16
LAG_X = 4
LAG_USE = 5
GELU_A = math.sqrt(2.0 / math.pi)
GELU_B = 0.044715 * GELU_A
A_SLOTS, B_SLOTS, C_SLOTS = 3, 3, 4


def layer_kernel(
    num_layers, seq, dim, heads, hd, ffn,
    x_hbm, wqkv, wo, w1, w2, g1_hbm, g2_hbm, out_ref,
    g1_ref, g2_ref, xs, acc, hid, part, recv_a, send_c, recv_c, ys0, ys1, mean0, sum1, sum2,
    a_buf, b_buf, c_buf,
    g_sem, x_sem, a_sem, b_sem, c_sem, sa, ra, sc, rc, sd, rd,
):
    dp = lax.axis_index("dp")
    tp = lax.axis_index("tp")
    core = lax.rem(tp, 2)
    sib = (dp, tp + 1 - 2 * core)
    pair = (dp, lax.rem(tp + 2, 4))
    half = seq // 2
    mine = pl.ds(pl.multiple_of(core * half, half), half)
    other = pl.ds(pl.multiple_of((1 - core) * half, half), half)
    nc = dim // WID
    qkv_tiles, up_tiles = heads * 3 * hd // 256, ffn // 256
    o_off = heads * 3 * hd

    barrier = pltpu.get_barrier_semaphore()
    for peer in (sib, pair):
        pl.semaphore_signal(barrier, inc=1, device_id=peer, device_id_type=MESH)

    def rows(j):
        return pl.ds(pl.multiple_of(j * WID, WID), WID)

    def x_copy(j):
        return pltpu.make_async_copy(x_hbm.at[:, rows(j)], xs.at[j], x_sem.at[j])

    def put_out(j):
        out_ref[:, rows(j)] = xs[j]

    def a_start(stage, j):
        layer, is_up = stage // 2, stage % 2
        if stage >= 2 * num_layers:
            return
        slot = lax.rem(stage * nc + j, A_SLOTS)
        if is_up:
            for t in range(up_tiles):
                pltpu.make_async_copy(
                    w1.at[layer, rows(j), pl.ds(t * 256, 256)], a_buf.at[slot, t], a_sem.at[slot]
                ).start(priority=1)
        else:
            for s in range(2):
                pltpu.make_async_copy(
                    wqkv.at[layer, :, s, rows(j), :],
                    a_buf.at[slot, pl.ds(0, qkv_tiles), :, pl.ds(s * 128, 128)],
                    a_sem.at[slot],
                ).start(priority=1)

    def a_next(stage, j):
        @pl.when(j + A_SLOTS < nc)
        def _():
            a_start(stage, j + A_SLOTS)

        @pl.when(j + A_SLOTS >= nc)
        def _():
            a_start(stage + 1, j + A_SLOTS - nc)

    def a_wait(stage, j):
        slot = lax.rem(stage * nc + j, A_SLOTS)
        tiles = up_tiles if stage % 2 else qkv_tiles
        view = a_buf.at[slot, pl.ds(0, tiles)]
        pltpu.make_async_copy(view, view, a_sem.at[slot]).wait()
        return slot

    def b_copy(layer, j):
        slot = lax.rem(layer * nc + j, B_SLOTS)
        return slot, pltpu.make_async_copy(
            w2.at[layer, :, rows(j)], b_buf.at[slot], b_sem.at[slot])

    def c_copy(layer, j):
        slot = lax.rem(layer * nc + j, C_SLOTS)
        return slot, pltpu.make_async_copy(
            wo.at[layer, :, rows(j)], c_buf.at[slot], c_sem.at[slot])

    def ring_next(copy, slots, priority, layer, j):
        @pl.when(j + slots < nc)
        def _():
            copy(layer, j + slots)[1].start(priority=priority)

        if layer + 1 < num_layers:
            @pl.when(j + slots >= nc)
            def _():
                copy(layer + 1, j + slots - nc)[1].start(priority=priority)

    def prep_start(j):
        m = jnp.mean(xs[j].astype(F32), axis=1, keepdims=True)
        mean0[...] = jnp.broadcast_to(m, mean0.shape)
        sum1[...] = jnp.zeros_like(sum1)
        sum2[...] = jnp.zeros_like(sum2)

    def prep(stage, j, y_ref):
        layer, is_up = stage // 2, stage % 2
        gain_ref = g2_ref if is_up else g1_ref
        gain = gain_ref[pl.ds(layer, 1), rows(j)]
        shift = mean0[...]
        s1, s2 = sum1[...], sum2[...]
        for t in range(WID // 128):
            cols = slice(t * 128, (t + 1) * 128)
            d = xs[j, :, cols].astype(F32) - shift
            s1 = s1 + d
            s2 = s2 + d * d
            y_ref[GAIN:, cols] = (d * gain[:, cols]).astype(BF16)
        sum1[...] = s1
        sum2[...] = s2
        g_hi = gain.astype(BF16)
        g_lo = (gain - g_hi.astype(F32)).astype(BF16)
        row = lax.broadcasted_iota(jnp.int32, (GAIN, WID), 0)
        hi = jnp.broadcast_to(g_hi.astype(F32), (GAIN, WID))
        lo = jnp.broadcast_to(g_lo.astype(F32), (GAIN, WID))
        extra = jnp.where(row == 0, hi, jnp.where(row == 1, lo, 0.0))
        y_ref[0:GAIN, :] = extra.astype(BF16)

    def mul(stage, slot, y_ref, piece=slice(None)):
        lhs = y_ref[...]
        for t in range(up_tiles if stage % 2 else qkv_tiles)[piece]:
            cols = slice(t * 256, (t + 1) * 256)
            acc[:, cols] += jnp.dot(lhs, a_buf[slot, t], preferred_element_type=F32)

    def mul_last(stage, slot, y_ref):
        layer, is_up = stage // 2, stage % 2
        delta = jnp.sum(sum1[...], axis=1, keepdims=True) * (1.0 / dim)
        var = jnp.sum(sum2[...], axis=1, keepdims=True) * (1.0 / dim) - delta * delta
        rstd = lax.rsqrt(jnp.maximum(var, 0.0) + 1e-5)
        if is_up:
            rstd = 0.5 * rstd
        back = delta * rstd
        lhs = y_ref[...]
        for t in range(up_tiles if is_up else qkv_tiles):
            cols = slice(t * 256, (t + 1) * 256)
            full = acc[:, cols] + jnp.dot(lhs, a_buf[slot, t], preferred_element_type=F32)
            colsum = full[0:1] + full[1:2]
            val = full[GAIN:] * rstd - back * colsum
            if is_up:
                inner = val * (2.0 * GELU_A + 8.0 * GELU_B * (val * val))
                val = val + val * jnp.tanh(inner)
            hid[:, cols] = val.astype(BF16)

    def use_first(stage, j):
        @pl.when(j == 0)
        def _():
            prep_start(j)

        prep(stage, j, ys0)
        mul(stage, a_wait(stage, j), ys0, slice(0, up_tiles // 2) if stage % 2 else slice(None))
        if stage % 2 == 0:
            a_next(stage, j)

    def use_second(stage, j):
        mul(stage, lax.rem(stage * nc + j, A_SLOTS), ys0, slice(up_tiles // 2, None))
        a_next(stage, j)

    def use_last(stage, j):
        prep(stage, j, ys0)
        mul_last(stage, a_wait(stage, j), ys0)
        a_next(stage, j)

    def attention():
        q_pos = lax.broadcasted_iota(jnp.int32, (seq, seq), 0)
        k_pos = lax.broadcasted_iota(jnp.int32, (seq, seq), 1)
        keep = k_pos <= q_pos
        scale = 1.0 / math.sqrt(hd)
        for h in range(heads):
            base = 3 * h * hd
            q = hid[:, base:base + hd]
            k = hid[:, base + hd:base + 2 * hd]
            v = hid[:, base + 2 * hd:base + 3 * hd]
            s = lax.dot_general(q, k, (((1,), (1,)), ((), ())), preferred_element_type=F32) * scale
            s = jnp.where(keep, s, -1e30)
            e = jnp.exp(s - jnp.max(s, axis=1, keepdims=True))
            total = jnp.sum(e, axis=1, keepdims=True)
            mix = jnp.dot(e.astype(BF16), v, preferred_element_type=F32)
            hid[:, o_off + h * hd:o_off + (h + 1) * hd] = (mix / total).astype(BF16)

    def make_out(layer, j):
        slot, copy = c_copy(layer, j)
        copy.wait()
        part[j] = jnp.dot(hid[:, o_off:], c_buf[slot], preferred_element_type=F32).astype(BF16)
        ring_next(c_copy, C_SLOTS, 0, layer, j)

    def make_down(layer, j):
        slot, copy = b_copy(layer, j)
        copy.wait()
        part[j] = jnp.dot(hid[...], b_buf[slot], preferred_element_type=F32).astype(BF16)
        ring_next(b_copy, B_SLOTS, 1, layer, j)

    def window(index, make, stage):
        par = index % 2

        def a_send(j):
            return pltpu.make_async_remote_copy(
                part.at[j, other], recv_a.at[par, j], sa.at[j], ra.at[par, j],
                device_id=sib, device_id_type=MESH)

        def c_send(j):
            return pltpu.make_async_remote_copy(
                send_c.at[j], recv_c.at[par, j], sc.at[j], rc.at[par, j],
                device_id=pair, device_id_type=MESH)

        def d_send(j):
            return pltpu.make_async_remote_copy(
                xs.at[j, mine], xs.at[j, mine], sd.at[j], rd.at[par, j],
                device_id=sib, device_id_type=MESH)

        def d_recv(j):
            return pltpu.make_async_remote_copy(
                xs.at[j, other], xs.at[j, other], sd.at[j], rd.at[par, j],
                device_id=sib, device_id_type=MESH)

        def pair_sum(j):
            a_send(j).wait_recv()
            send_c[j] = (part[j, mine, :].astype(F32) + recv_a[par, j].astype(F32)).astype(BF16)
            c_send(j).start()

        def finish(j):
            a_send(j).wait_send()
            c_send(j).wait_send()
            d_send(j).wait_send()
            d_recv(j).wait_recv()

        def step(i, carry):
            @pl.when(i < nc)
            def _():
                make(i)
                a_send(i).start()

            @pl.when(i == 0)
            def _():
                if stage is not None:
                    acc[...] = jnp.zeros_like(acc)
                pair_sum(0)

            @pl.when(jnp.logical_and(i >= 2, i < nc + 1))
            def _():
                pair_sum(i - 1)

            used = i - LAG_USE
            if stage is not None and stage % 2:
                @pl.when(jnp.logical_and(used >= 0, used < nc - 1))
                def _():
                    finish(used)
                    use_first(stage, used)

            @pl.when(jnp.logical_and(i >= LAG_X, i < nc + LAG_X))
            def _():
                j = i - LAG_X
                c_send(j).wait_recv()
                total = send_c[j].astype(F32) + recv_c[par, j].astype(F32)
                xs[j, mine, :] = (xs[j, mine, :].astype(F32) + total).astype(BF16)
                d_send(j).start()

            if stage is not None:
                @pl.when(jnp.logical_and(used >= 0, used < nc - 1))
                def _():
                    if stage % 2:
                        use_second(stage, used)
                    else:
                        finish(used)
                        use_first(stage, used)

                @pl.when(used == nc - 1)
                def _():
                    finish(used)
                    use_last(stage, used)
            else:
                @pl.when(used >= 0)
                def _():
                    finish(used)
                    put_out(used)
            return carry

        lax.fori_loop(0, nc + LAG_USE, step, 0)

    x_copy(0).start()
    g_copies = [pltpu.make_async_copy(src, dst, g_sem.at[n])
                for n, (src, dst) in enumerate(((g1_hbm, g1_ref), (g2_hbm, g2_ref)))]
    for copy in g_copies:
        copy.start()
    a_start(0, 0)
    for j in range(1, nc):
        x_copy(j).start()
    for j in range(1, A_SLOTS):
        a_start(0, j)
    acc[...] = jnp.zeros_like(acc)
    for copy in g_copies:
        copy.wait()
    x_copy(0).wait()
    prep_start(0)
    prep(0, 0, ys0)

    def first(j, now, then):
        x_copy(j + 1).wait()
        slot = a_wait(0, j)
        prep(0, j + 1, then)
        mul(0, slot, now)
        a_next(0, j)

    def first_two(i, carry):
        first(2 * i, ys0, ys1)
        first(2 * i + 1, ys1, ys0)
        return carry

    lax.fori_loop(0, nc // 2 - 1, first_two, 0)
    for n in range(C_SLOTS):
        c_copy(0, n)[1].start()
    first(nc - 2, ys0, ys1)
    mul_last(0, a_wait(0, nc - 1), ys1)
    a_next(0, nc - 1)
    attention()
    for j in range(B_SLOTS):
        b_copy(0, j)[1].start(priority=1)
    pl.semaphore_wait(barrier, 2)

    for layer in range(num_layers):
        window(2 * layer, functools.partial(make_out, layer), 2 * layer + 1)
        if layer + 1 < num_layers:
            window(2 * layer + 1, functools.partial(make_down, layer), 2 * layer + 2)
            attention()
        else:
            window(2 * layer + 1, functools.partial(make_down, layer), None)


def solution(mesh):
    def device_fn(act_in, w_qkv, w_out, w_up, w_down, gain_one, gain_two):
        seq, dim = act_in.shape
        num_layers, _, heads, _, hd = w_qkv.shape
        ffn = w_up.shape[2]
        nc = dim // WID
        wq = jnp.transpose(w_qkv, (0, 2, 3, 1, 4)).reshape(num_layers, heads * 3 // 2, 2, dim, hd)
        wo = w_out.reshape(num_layers, heads * hd, dim)
        any_spec = pl.BlockSpec(memory_space=pl.ANY)
        return pl.pallas_call(
            functools.partial(layer_kernel, num_layers, seq, dim, heads, hd, ffn),
            out_shape=pltpu.VMEM((seq, dim), BF16),
            in_specs=[any_spec] * 7,
            out_specs=pl.BlockSpec(memory_space=pltpu.VMEM),
            scratch_shapes=[
                pltpu.VMEM((num_layers, dim), F32),
                pltpu.VMEM((num_layers, dim), F32),
                pltpu.VMEM((nc, seq, WID), BF16),
                pltpu.VMEM((seq + GAIN, ffn), F32),
                pltpu.VMEM((seq, ffn), BF16),
                pltpu.VMEM((nc, seq, WID), BF16),
                pltpu.VMEM((2, nc, seq // 2, WID), BF16),
                pltpu.VMEM((nc, seq // 2, WID), BF16),
                pltpu.VMEM((2, nc, seq // 2, WID), BF16),
                pltpu.VMEM((seq + GAIN, WID), BF16),
                pltpu.VMEM((seq + GAIN, WID), BF16),
                pltpu.VMEM((seq, 128), F32),
                pltpu.VMEM((seq, 128), F32),
                pltpu.VMEM((seq, 128), F32),
                pltpu.VMEM((A_SLOTS, ffn // 256, WID, 256), BF16),
                pltpu.VMEM((B_SLOTS, ffn, WID), BF16),
                pltpu.VMEM((C_SLOTS, heads * hd, WID), BF16),
                pltpu.SemaphoreType.DMA((2,)),
                pltpu.SemaphoreType.DMA((nc,)),
                pltpu.SemaphoreType.DMA((A_SLOTS,)),
                pltpu.SemaphoreType.DMA((B_SLOTS,)),
                pltpu.SemaphoreType.DMA((C_SLOTS,)),
                pltpu.SemaphoreType.DMA((nc,)),
                pltpu.SemaphoreType.DMA((2, nc)),
                pltpu.SemaphoreType.DMA((nc,)),
                pltpu.SemaphoreType.DMA((2, nc)),
                pltpu.SemaphoreType.DMA((nc,)),
                pltpu.SemaphoreType.DMA((2, nc)),
            ],
            compiler_params=pltpu.CompilerParams(
                collective_id=0, has_side_effects=True, vmem_limit_bytes=62_000_000),
            name="layers",
        )(act_in, wq, wo, w_up, w_down, gain_one, gain_two)

    return jax.shard_map(
        device_fn,
        mesh=mesh,
        in_specs=(
            P("dp", None),
            P(None, None, "tp", None, None),
            P(None, "tp", None, None),
            P(None, None, "tp"),
            P(None, "tp", None),
            P(None, None),
            P(None, None),
        ),
        out_specs=P("dp", None),
        check_vma=False,
    )
```

```python
import functools
import math
import jax
import jax.numpy as jnp
from jax import lax
from jax.experimental import pallas as pl
from jax.experimental.pallas import tpu as pltpu
from jax.sharding import PartitionSpec as P

MESH = pl.DeviceIdType.MESH
F32, BF16 = jnp.float32, jnp.bfloat16
WID = 512
GAIN = 16
LAG_X = 4
LAG_USE = 5
GELU_A = math.sqrt(2.0 / math.pi)
GELU_B = 0.044715 * GELU_A
A_SLOTS, B_SLOTS, C_SLOTS = 3, 3, 4


def layer_kernel(
    num_layers, seq, dim, heads, hd, ffn,
    x_hbm, wqkv, wo, w1, w2, g1_hbm, g2_hbm, out_ref,
    g1_ref, g2_ref, xs, acc, hid, part, recv_a, send_c, recv_c, ys0, ys1, mean0, sum1, sum2,
    a_buf, b_buf, c_buf,
    g_sem, x_sem, a_sem, b_sem, c_sem, sa, ra, sc, rc, sd, rd,
):
    dp = lax.axis_index("dp")
    tp = lax.axis_index("tp")
    core = lax.rem(tp, 2)
    sib = (dp, tp + 1 - 2 * core)
    pair = (dp, lax.rem(tp + 2, 4))
    half = seq // 2
    mine = pl.ds(pl.multiple_of(core * half, half), half)
    other = pl.ds(pl.multiple_of((1 - core) * half, half), half)
    nc = dim // WID
    qkv_tiles, up_tiles = heads * 3 * hd // 256, ffn // 256
    o_off = heads * 3 * hd

    barrier = pltpu.get_barrier_semaphore()
    for peer in (sib, pair):
        pl.semaphore_signal(barrier, inc=1, device_id=peer, device_id_type=MESH)

    def rows(j):
        return pl.ds(pl.multiple_of(j * WID, WID), WID)

    def x_copy(j):
        return pltpu.make_async_copy(x_hbm.at[:, rows(j)], xs.at[j], x_sem.at[j])

    def put_out(j):
        out_ref[:, rows(j)] = xs[j]

    def a_start(stage, j):
        layer, is_up = stage // 2, stage % 2
        if stage >= 2 * num_layers:
            return
        slot = lax.rem(stage * nc + j, A_SLOTS)
        if is_up:
            for t in range(up_tiles):
                pltpu.make_async_copy(
                    w1.at[layer, rows(j), pl.ds(t * 256, 256)], a_buf.at[slot, t], a_sem.at[slot]
                ).start(priority=1)
        else:
            for s in range(2):
                pltpu.make_async_copy(
                    wqkv.at[layer, :, s, rows(j), :],
                    a_buf.at[slot, pl.ds(0, qkv_tiles), :, pl.ds(s * 128, 128)],
                    a_sem.at[slot],
                ).start(priority=1)

    def a_next(stage, j):
        @pl.when(j + A_SLOTS < nc)
        def _():
            a_start(stage, j + A_SLOTS)

        @pl.when(j + A_SLOTS >= nc)
        def _():
            a_start(stage + 1, j + A_SLOTS - nc)

    def a_wait(stage, j):
        slot = lax.rem(stage * nc + j, A_SLOTS)
        tiles = up_tiles if stage % 2 else qkv_tiles
        view = a_buf.at[slot, pl.ds(0, tiles)]
        pltpu.make_async_copy(view, view, a_sem.at[slot]).wait()
        return slot

    def b_copy(layer, j):
        slot = lax.rem(layer * nc + j, B_SLOTS)
        return slot, pltpu.make_async_copy(
            w2.at[layer, :, rows(j)], b_buf.at[slot], b_sem.at[slot])

    def c_copy(layer, j):
        slot = lax.rem(layer * nc + j, C_SLOTS)
        return slot, pltpu.make_async_copy(
            wo.at[layer, :, rows(j)], c_buf.at[slot], c_sem.at[slot])

    def ring_next(copy, slots, priority, layer, j):
        @pl.when(j + slots < nc)
        def _():
            copy(layer, j + slots)[1].start(priority=priority)

        if layer + 1 < num_layers:
            @pl.when(j + slots >= nc)
            def _():
                copy(layer + 1, j + slots - nc)[1].start(priority=priority)

    def prep_start(j):
        m = jnp.mean(xs[j].astype(F32), axis=1, keepdims=True)
        mean0[...] = jnp.broadcast_to(m, mean0.shape)
        sum1[...] = jnp.zeros_like(sum1)
        sum2[...] = jnp.zeros_like(sum2)

    def prep(stage, j, y_ref):
        layer, is_up = stage // 2, stage % 2
        gain_ref = g2_ref if is_up else g1_ref
        gain = gain_ref[pl.ds(layer, 1), rows(j)]
        shift = mean0[...]
        s1, s2 = sum1[...], sum2[...]
        for t in range(WID // 128):
            cols = slice(t * 128, (t + 1) * 128)
            d = xs[j, :, cols].astype(F32) - shift
            s1 = s1 + d
            s2 = s2 + d * d
            y_ref[GAIN:, cols] = (d * gain[:, cols]).astype(BF16)
        sum1[...] = s1
        sum2[...] = s2
        g_hi = gain.astype(BF16)
        g_lo = (gain - g_hi.astype(F32)).astype(BF16)
        row = lax.broadcasted_iota(jnp.int32, (GAIN, WID), 0)
        hi = jnp.broadcast_to(g_hi.astype(F32), (GAIN, WID))
        lo = jnp.broadcast_to(g_lo.astype(F32), (GAIN, WID))
        extra = jnp.where(row == 0, hi, jnp.where(row == 1, lo, 0.0))
        y_ref[0:GAIN, :] = extra.astype(BF16)

    def mul(stage, slot, y_ref, piece=slice(None), fresh=False):
        lhs = y_ref[...]
        for t in range(up_tiles if stage % 2 else qkv_tiles)[piece]:
            cols = slice(t * 256, (t + 1) * 256)
            term = jnp.dot(lhs, a_buf[slot, t], preferred_element_type=F32)
            acc[:, cols] = term if fresh else acc[:, cols] + term

    def mul_last(stage, slot, y_ref):
        layer, is_up = stage // 2, stage % 2
        delta = jnp.sum(sum1[...], axis=1, keepdims=True) * (1.0 / dim)
        var = jnp.sum(sum2[...], axis=1, keepdims=True) * (1.0 / dim) - delta * delta
        rstd = lax.rsqrt(jnp.maximum(var, 0.0) + 1e-5)
        if is_up:
            rstd = 0.5 * rstd
        back = delta * rstd
        lhs = y_ref[...]
        for t in range(up_tiles if is_up else qkv_tiles):
            cols = slice(t * 256, (t + 1) * 256)
            full = acc[:, cols] + jnp.dot(lhs, a_buf[slot, t], preferred_element_type=F32)
            colsum = full[0:1] + full[1:2]
            val = full[GAIN:] * rstd - back * colsum
            if is_up:
                inner = val * (2.0 * GELU_A + 8.0 * GELU_B * (val * val))
                val = val + val * jnp.tanh(inner)
            hid[:, cols] = val.astype(BF16)

    def use_first(stage, j):
        @pl.when(j == 0)
        def _():
            prep_start(j)

        prep(stage, j, ys0)
        slot = a_wait(stage, j)
        if stage % 2:
            mul(stage, slot, ys0, slice(0, up_tiles // 2))
        else:
            pl.when(j == 0)(lambda: mul(stage, slot, ys0, fresh=True))
            pl.when(j > 0)(lambda: mul(stage, slot, ys0))
            a_next(stage, j)

    def use_second(stage, j):
        mul(stage, lax.rem(stage * nc + j, A_SLOTS), ys0, slice(up_tiles // 2, None))
        a_next(stage, j)

    def use_last(stage, j):
        prep(stage, j, ys0)
        mul_last(stage, a_wait(stage, j), ys0)
        a_next(stage, j)

    def attention():
        q_pos = lax.broadcasted_iota(jnp.int32, (seq, seq), 0)
        k_pos = lax.broadcasted_iota(jnp.int32, (seq, seq), 1)
        keep = k_pos <= q_pos
        scale = 1.0 / math.sqrt(hd)
        for h in range(heads):
            base = 3 * h * hd
            q = hid[:, base:base + hd]
            k = hid[:, base + hd:base + 2 * hd]
            v = hid[:, base + 2 * hd:base + 3 * hd]
            s = lax.dot_general(q, k, (((1,), (1,)), ((), ())), preferred_element_type=F32) * scale
            s = jnp.where(keep, s, -1e30)
            e = jnp.exp(s - jnp.max(s, axis=1, keepdims=True))
            total = jnp.sum(e, axis=1, keepdims=True)
            mix = jnp.dot(e.astype(BF16), v, preferred_element_type=F32)
            hid[:, o_off + h * hd:o_off + (h + 1) * hd] = (mix / total).astype(BF16)

    def make_out(layer, j):
        slot, copy = c_copy(layer, j)
        copy.wait()
        part[j] = jnp.dot(hid[:, o_off:], c_buf[slot], preferred_element_type=F32).astype(BF16)
        ring_next(c_copy, C_SLOTS, 0, layer, j)

    def make_down(layer, j):
        slot, copy = b_copy(layer, j)
        copy.wait()
        part[j] = jnp.dot(hid[...], b_buf[slot], preferred_element_type=F32).astype(BF16)
        ring_next(b_copy, B_SLOTS, 1, layer, j)

    def make_down_half(layer, n):
        slot = lax.rem(layer * nc, B_SLOTS)
        if n == 0:
            b_copy(layer, 0)[1].wait()
        cols = slice(n * WID // 2, (n + 1) * WID // 2)
        for lo in (0, half):
            block = slice(lo, lo + half)
            part[0, block, cols] = jnp.dot(
                hid[block, :], b_buf[slot, :, cols], preferred_element_type=F32).astype(BF16)

    def window(index, make, stage):
        par = index % 2
        layer, halved = index // 2, index % 2 == 1

        def a_send(j):
            return pltpu.make_async_remote_copy(
                part.at[j, other], recv_a.at[par, j], sa.at[j], ra.at[par, j],
                device_id=sib, device_id_type=MESH)

        def c_send(j):
            return pltpu.make_async_remote_copy(
                send_c.at[j], recv_c.at[par, j], sc.at[j], rc.at[par, j],
                device_id=pair, device_id_type=MESH)

        def d_send(j):
            return pltpu.make_async_remote_copy(
                xs.at[j, mine], xs.at[j, mine], sd.at[j], rd.at[par, j],
                device_id=sib, device_id_type=MESH)

        def d_recv(j):
            return pltpu.make_async_remote_copy(
                xs.at[j, other], xs.at[j, other], sd.at[j], rd.at[par, j],
                device_id=sib, device_id_type=MESH)

        def a_half(n):
            cols = pl.ds(n * WID // 2, WID // 2)
            return pltpu.make_async_remote_copy(
                part.at[0, other, cols], recv_a.at[par, 0, :, cols], sa.at[0], ra.at[par, n * nc],
                device_id=sib, device_id_type=MESH)

        def half_sum(n):
            cols = slice(n * WID // 2, (n + 1) * WID // 2)
            a_half(n).wait_recv()
            total = part[0, mine, cols].astype(F32) + recv_a[par, 0, :, cols].astype(F32)
            send_c[0, :, cols] = total.astype(BF16)
            cols = pl.ds(n * WID // 2, WID // 2)
            pltpu.make_async_remote_copy(
                send_c.at[0, :, cols], recv_c.at[par, 0, :, cols], sc.at[0], rc.at[par, 0],
                device_id=pair, device_id_type=MESH).start()

        def pair_sum(j):
            a_send(j).wait_recv()
            send_c[j] = (part[j, mine, :].astype(F32) + recv_a[par, j].astype(F32)).astype(BF16)
            c_send(j).start()

        def finish(j):
            a_send(j).wait_send()
            c_send(j).wait_send()
            d_send(j).wait_send()
            d_recv(j).wait_recv()

        def step(i, carry):
            if halved:
                @pl.when(i == 0)
                def _():
                    make_down_half(layer, 0)
                    a_half(0).start()

                @pl.when(i == 0)
                def _():
                    make_down_half(layer, 1)
                    a_half(1).start()
                    ring_next(b_copy, B_SLOTS, 1, layer, 0)
                    half_sum(0)

            @pl.when(jnp.logical_and(i >= halved, i < nc))
            def _():
                make(i)
                a_send(i).start()

            if halved:
                pl.when(i == 1)(lambda: half_sum(1))
            else:
                @pl.when(i == 0)
                def _():
                    acc[...] = jnp.zeros_like(acc)
                    pair_sum(0)

            @pl.when(jnp.logical_and(i >= 2, i < nc + 1))
            def _():
                pair_sum(i - 1)

            used = i - LAG_USE
            if stage is not None and stage % 2:
                @pl.when(jnp.logical_and(used >= 0, used < nc - 1))
                def _():
                    finish(used)
                    use_first(stage, used)

            @pl.when(jnp.logical_and(i >= LAG_X, i < nc + LAG_X))
            def _():
                j = i - LAG_X
                c_send(j).wait_recv()
                total = send_c[j].astype(F32) + recv_c[par, j].astype(F32)
                xs[j, mine, :] = (xs[j, mine, :].astype(F32) + total).astype(BF16)
                d_send(j).start()

            if stage is not None:
                @pl.when(jnp.logical_and(used >= 0, used < nc - 1))
                def _():
                    if stage % 2:
                        use_second(stage, used)
                    else:
                        finish(used)
                        use_first(stage, used)

                @pl.when(used == nc - 1)
                def _():
                    finish(used)
                    use_last(stage, used)
            else:
                @pl.when(used >= 0)
                def _():
                    finish(used)
                    put_out(used)
            return carry

        lax.fori_loop(0, nc + LAG_USE, step, 0)

    x_copy(0).start()
    g_copies = [pltpu.make_async_copy(src, dst, g_sem.at[n])
                for n, (src, dst) in enumerate(((g1_hbm, g1_ref), (g2_hbm, g2_ref)))]
    for copy in g_copies:
        copy.start()
    a_start(0, 0)
    for j in range(1, nc):
        x_copy(j).start()
    for j in range(1, A_SLOTS):
        a_start(0, j)
    acc[...] = jnp.zeros_like(acc)
    for copy in g_copies:
        copy.wait()
    x_copy(0).wait()
    prep_start(0)
    prep(0, 0, ys0)

    def first(j, now, then):
        x_copy(j + 1).wait()
        slot = a_wait(0, j)
        prep(0, j + 1, then)
        mul(0, slot, now)
        a_next(0, j)

    def first_two(i, carry):
        first(2 * i, ys0, ys1)
        first(2 * i + 1, ys1, ys0)
        return carry

    lax.fori_loop(0, nc // 2 - 1, first_two, 0)
    for n in range(C_SLOTS):
        c_copy(0, n)[1].start()
    first(nc - 2, ys0, ys1)
    mul_last(0, a_wait(0, nc - 1), ys1)
    a_next(0, nc - 1)
    attention()
    for j in range(B_SLOTS):
        b_copy(0, j)[1].start(priority=1)
    pl.semaphore_wait(barrier, 2)

    for layer in range(num_layers):
        window(2 * layer, functools.partial(make_out, layer), 2 * layer + 1)
        if layer + 1 < num_layers:
            window(2 * layer + 1, functools.partial(make_down, layer), 2 * layer + 2)
            attention()
        else:
            window(2 * layer + 1, functools.partial(make_down, layer), None)


def solution(mesh):
    def device_fn(act_in, w_qkv, w_out, w_up, w_down, gain_one, gain_two):
        seq, dim = act_in.shape
        num_layers, _, heads, _, hd = w_qkv.shape
        ffn = w_up.shape[2]
        nc = dim // WID
        wq = jnp.transpose(w_qkv, (0, 2, 3, 1, 4)).reshape(num_layers, heads * 3 // 2, 2, dim, hd)
        wo = w_out.reshape(num_layers, heads * hd, dim)
        any_spec = pl.BlockSpec(memory_space=pl.ANY)
        return pl.pallas_call(
            functools.partial(layer_kernel, num_layers, seq, dim, heads, hd, ffn),
            out_shape=pltpu.VMEM((seq, dim), BF16),
            in_specs=[any_spec] * 7,
            out_specs=pl.BlockSpec(memory_space=pltpu.VMEM),
            scratch_shapes=[
                pltpu.VMEM((num_layers, dim), F32),
                pltpu.VMEM((num_layers, dim), F32),
                pltpu.VMEM((nc, seq, WID), BF16),
                pltpu.VMEM((seq + GAIN, ffn), F32),
                pltpu.VMEM((seq, ffn), BF16),
                pltpu.VMEM((nc, seq, WID), BF16),
                pltpu.VMEM((2, nc, seq // 2, WID), BF16),
                pltpu.VMEM((nc, seq // 2, WID), BF16),
                pltpu.VMEM((2, nc, seq // 2, WID), BF16),
                pltpu.VMEM((seq + GAIN, WID), BF16),
                pltpu.VMEM((seq + GAIN, WID), BF16),
                pltpu.VMEM((seq, 128), F32),
                pltpu.VMEM((seq, 128), F32),
                pltpu.VMEM((seq, 128), F32),
                pltpu.VMEM((A_SLOTS, ffn // 256, WID, 256), BF16),
                pltpu.VMEM((B_SLOTS, ffn, WID), BF16),
                pltpu.VMEM((C_SLOTS, heads * hd, WID), BF16),
                pltpu.SemaphoreType.DMA((2,)),
                pltpu.SemaphoreType.DMA((nc,)),
                pltpu.SemaphoreType.DMA((A_SLOTS,)),
                pltpu.SemaphoreType.DMA((B_SLOTS,)),
                pltpu.SemaphoreType.DMA((C_SLOTS,)),
                pltpu.SemaphoreType.DMA((nc,)),
                pltpu.SemaphoreType.DMA((2, nc + 1)),
                pltpu.SemaphoreType.DMA((nc,)),
                pltpu.SemaphoreType.DMA((2, nc)),
                pltpu.SemaphoreType.DMA((nc,)),
                pltpu.SemaphoreType.DMA((2, nc)),
            ],
            compiler_params=pltpu.CompilerParams(
                collective_id=0, has_side_effects=True, vmem_limit_bytes=62_000_000),
            name="layers",
        )(act_in, wq, wo, w_up, w_down, gain_one, gain_two)

    return jax.shard_map(
        device_fn,
        mesh=mesh,
        in_specs=(
            P("dp", None),
            P(None, None, "tp", None, None),
            P(None, "tp", None, None),
            P(None, None, "tp"),
            P(None, "tp", None),
            P(None, None),
            P(None, None),
        ),
        out_specs=P("dp", None),
        check_vma=False,
    )
```
